32 devices in a mesh: dp: 4 (over z), sp: 8 (over y, x, core).
Axes of the slice: x: 2, y: 2, z: 4, core: 2. Of those that a mesh axis runs over, the one named last changes fastest.
Arguments:
- queries_in: bfloat16 [8, 8192, 16, 128], P('dp', 'sp'), may hold values from -6 to 6
- keys_in: bfloat16 [8, 8192, 16, 128], P('dp', 'sp'), may hold values from -6 to 6
- values_in: bfloat16 [8, 8192, 16, 128], P('dp', 'sp'), may hold values from -6 to 6
- out_weight: bfloat16 [2048, 2048], P('dp'), may hold values from -0.125 to 0.125
Outputs:
- block_out: bfloat16 [8, 8192, 2048], P('dp', 'sp')
The draws below stay inside these ranges and needn't reach their ends.
All inputs are finite; a program needn't handle non-finite values.
Results may differ from the reference program's by a relative error of at most 0.006.
Values may be sent and summed in bfloat16 or wider, within the bound.
A program may use at most 320 MiB of HBM per device.

```python
import jax
import jax.numpy as jnp
from jax import lax

HEADS = 16
HEAD_SIZE = 128
BATCH = 8
TOKENS = 8192
WIDTH = 2048


def block_levels(own_key, dims, cuts, least, top_value):
    def one(dim, shards_of):
        draws = jax.random.uniform(jax.random.fold_in(jax.random.fold_in(own_key, 6), dim), (shards_of,), jnp.float32, least / len(cuts), top_value / len(cuts))
        return jnp.repeat(jnp.exp(draws), dims[dim] // shards_of).reshape((-1,) + (1,) * (len(dims) - dim - 1))

    gain = one(*cuts[0])
    for cut in cuts[1:]:
        gain = gain * one(*cut)
    return gain


def bell_draw(key, extent, deviation, limit, cuts=(), kind=jnp.bfloat16):
    loudness = block_levels(key, extent, cuts, -0.22, 0.18) if cuts else 1.0
    drawn = jax.random.normal(key, extent, jnp.float32) * deviation * loudness
    return jnp.minimum(jnp.maximum(drawn, -limit), limit).astype(kind)


def setup_inputs(seed: int = 0) -> dict:
    key_list = jax.random.split(jax.random.key(seed), 5)
    queries_in = bell_draw(key_list[0], (BATCH, TOKENS, HEADS, HEAD_SIZE), 1.0, 6.0, ((0, 4), (1, 8)))
    keys_in = bell_draw(key_list[1], (BATCH, TOKENS, HEADS, HEAD_SIZE), 1.0, 6.0, ((0, 4), (1, 8)))
    values_in = bell_draw(key_list[2], (BATCH, TOKENS, HEADS, HEAD_SIZE), 1.0, 6.0, ((0, 4), (1, 8)))
    out_weight = bell_draw(key_list[3], (WIDTH, WIDTH), WIDTH ** -0.5, 0.125, ((0, 4),))
    return dict(queries_in=queries_in, keys_in=keys_in, values_in=values_in, out_weight=out_weight)


def feature_map(values):
    wide = values.astype(jnp.float32)
    return (wide * wide + 0.1).astype(jnp.bfloat16)


def finish_heads(read, count):
    result = read * count ** 0.5
    return result.astype(jnp.bfloat16)


def look_up(features, state, mass):
    small = lax.optimization_barrier(state.astype(jnp.bfloat16))
    top = jnp.einsum("bthd,bhde->bthe", features.astype(jnp.float32), small.astype(jnp.float32))
    bottom = jnp.einsum("bthd,bhd->bth", features.astype(jnp.float32), mass, precision=lax.Precision.HIGHEST)
    return top / (bottom + 1e-3)[..., None]


def reference(queries_in, keys_in, values_in, out_weight):
    query_feature, key_feature = lax.optimization_barrier((feature_map(queries_in), feature_map(keys_in)))
    state = jnp.einsum("bthd,bthe->bhde", key_feature.astype(jnp.float32), values_in.astype(jnp.float32)) / TOKENS
    mass = jnp.sum(key_feature.astype(jnp.float32), axis=1) / TOKENS
    mixed = finish_heads(look_up(query_feature, state, mass), TOKENS).reshape(BATCH, TOKENS, WIDTH)
    mixed = lax.optimization_barrier(mixed)
    block_out = jnp.einsum("btw,wv->btv", mixed.astype(jnp.float32), out_weight.astype(jnp.float32)).astype(jnp.bfloat16)
    return block_out
```

```python
import functools

import jax
import jax.numpy as jnp
from jax import lax
from jax.experimental import pallas as pl
from jax.experimental.pallas import tpu as pltpu
from jax.sharding import PartitionSpec as P

MESH = pl.DeviceIdType.MESH
SLOTS = 3
CHUNK = 256
TILE = 256


def feature_map(values):
    wide = values.astype(jnp.float32)
    return (wide * wide + 0.1).astype(jnp.bfloat16)


def gather_kernel(
    groups, count, chunk, batch, tokens, heads, size,
    k_ref, v_ref, w_ref, state_ref, mass_ref, wide_ref,
    k_buf, v_buf, total, sums, core_in, half_out, half_in, sums_out, sums_in,
    load_sem, own_sem, z_send, z_recv, w_send, w_recv, s_send, s_recv,
):
    depth, lanes = groups
    places = lanes // 2
    levels = places.bit_length() - 1
    d, s = lax.axis_index("dp"), lax.axis_index("sp")
    core, place = s % 2, s // 2
    piece = core * places + place
    rows = w_ref.shape[0]
    part = rows // lanes
    half_width = w_ref.shape[1] // 2
    steps = batch * tokens // chunk
    per_batch = tokens // chunk

    def flip(value, bit):
        return value + (1 << bit) - 2 * (1 << bit) * ((value // (1 << bit)) % 2)

    partners = [flip(s, bit) for bit in range(levels + 1)]

    def to_lane(bit):
        return {"sp": partners[bit]}

    barrier = pltpu.get_barrier_semaphore()
    for bit in range(levels + 1):
        pl.semaphore_signal(barrier, inc=1, device_id=to_lane(bit), device_id_type=MESH)
    for k in range(1, depth):
        pl.semaphore_signal(
            barrier, inc=1, device_id={"dp": (d + k) % depth}, device_id_type=MESH
        )

    def load(i):
        half = steps // 2
        side = jnp.where(i < half, 1 - core, core)
        at = side * half + i % half
        b, t = at // per_batch, at % per_batch
        slot = i % SLOTS
        return (
            pltpu.make_async_copy(
                k_ref.at[b, pl.ds(t * chunk, chunk)], k_buf.at[slot], load_sem.at[0, slot]
            ),
            pltpu.make_async_copy(
                v_ref.at[b, pl.ds(t * chunk, chunk)], v_buf.at[slot], load_sem.at[1, slot]
            ),
        )

    for i in range(min(SLOTS - 1, steps)):
        for copy in load(i):
            copy.start()
    total[...] = jnp.zeros_like(total)
    sums[...] = jnp.zeros_like(sums)
    pl.semaphore_wait(barrier, levels + depth)

    def z_copy(k):
        return pltpu.make_async_remote_copy(
            src_ref=w_ref.at[pl.ds(piece * part, part)],
            dst_ref=wide_ref.at[pl.ds(d * rows + piece * part, part)],
            send_sem=z_send.at[k],
            recv_sem=z_recv.at[k],
            device_id={"dp": (d + k) % depth},
            device_id_type=MESH,
        )

    near = []
    for k in range(1, depth // 2 + 1):
        near += [k] if k == depth - k else [k, depth - k]
    for k in near:
        z_copy(k).start()
    own = pltpu.make_async_copy(w_ref, wide_ref.at[pl.ds(d * rows, rows)], own_sem)
    own.start()

    def orders(side):
        return list(range(levels)) if side == 0 else list(range(levels))[::-1]

    def w_copies(k, stage):
        first = ((d - k) % depth) * rows
        if stage == levels:
            block = wide_ref.at[pl.ds(first + core * places * part, places * part)]
            slot = 2 * (places - 1)
            return [
                pltpu.make_async_remote_copy(
                    src_ref=block, dst_ref=block, send_sem=w_send.at[k, slot],
                    recv_sem=w_recv.at[k, slot], device_id=to_lane(0), device_id_type=MESH,
                )
            ]
        copies = []
        for side in range(2):
            bits = orders(side)
            for subset in range(1 << stage):
                member = place
                for j in range(stage):
                    if subset >> j & 1:
                        member = flip(member, bits[j])
                slot = side * (places - 1) + (1 << stage) - 1 + subset
                block = wide_ref.at[
                    pl.ds(first + (core * places + member) * part, part),
                    pl.ds(side * half_width, half_width),
                ]
                copies.append(
                    pltpu.make_async_remote_copy(
                        src_ref=block, dst_ref=block, send_sem=w_send.at[k, slot],
                        recv_sem=w_recv.at[k, slot], device_id=to_lane(bits[stage] + 1),
                        device_id_type=MESH,
                    )
                )
        return copies

    def w_step(k, stage):
        if stage == 0:
            z_copy(k).wait_recv()
        else:
            for copy in w_copies(k, stage - 1):
                copy.wait_recv()
        for copy in w_copies(k, stage):
            copy.start()

    held = total.shape[0] // 2
    core_copy = pltpu.make_async_remote_copy(
        src_ref=total.at[pl.ds((1 - core) * held, held)], dst_ref=core_in,
        send_sem=s_send.at[0], recv_sem=s_recv.at[0],
        device_id=to_lane(0), device_id_type=MESH,
    )

    def step(i, carry):
        @pl.when(i + SLOTS - 1 < steps)
        def _():
            for copy in load(i + SLOTS - 1):
                copy.start()

        @pl.when(i == steps // 2)
        def _():
            core_copy.start()

        for copy in load(i):
            copy.wait()
        slot = i % SLOTS
        half = steps // 2
        b = (jnp.where(i < half, 1 - core, core) * half + i % half) // per_batch
        k_feature = feature_map(k_buf[slot])
        sums[pl.ds(b * heads, heads), :] += jnp.sum(k_feature.astype(jnp.float32), axis=0)
        k_heads = pltpu.einshape("thd->htd", k_feature)
        v_heads = pltpu.einshape("thd->htd", v_buf[slot])
        for h in range(heads):
            at = pl.ds((b * heads + h) * size, size)
            total[at, :] += lax.dot_general(
                k_heads[h], v_heads[h], (((0,), (0,)), ((), ())),
                preferred_element_type=jnp.float32,
            )
        return carry

    lax.fori_loop(0, steps, step, 0)

    def mass_copy(stage):
        bit = 0 if stage == 0 else orders(0)[stage - 1] + 1
        return pltpu.make_async_remote_copy(
            src_ref=sums_out.at[stage], dst_ref=sums_in.at[stage],
            send_sem=s_send.at[1 + stage], recv_sem=s_recv.at[1 + stage],
            device_id=to_lane(bit), device_id_type=MESH,
        )

    def mass_send(stage):
        sums_out[stage] = sums[...]
        mass_copy(stage).start()

    def mass_take(stage):
        mass_copy(stage).wait()
        sums[...] += sums_in[stage]

    mass_send(0)
    core_copy.wait()
    mine = pl.ds(core * held, held)
    total[mine, :] += core_in[...]
    mass_take(0)

    quarter = held // 2
    starts = [[core * held + side * quarter] for side in range(2)]

    def reduce_copy(stage, side):
        length = quarter >> (stage + 1)
        slot = 2 + levels + 2 * stage + side
        base = side * quarter + quarter - 2 * length
        return pltpu.make_async_remote_copy(
            src_ref=half_out.at[pl.ds(base, length)], dst_ref=half_in.at[pl.ds(base, length)],
            send_sem=s_send.at[slot], recv_sem=s_recv.at[slot],
            device_id=to_lane(orders(side)[stage] + 1), device_id_type=MESH,
        )

    def reduce_send(stage):
        length = quarter >> (stage + 1)
        for side in range(2):
            first = starts[side][stage]
            upper = (place // (1 << orders(side)[stage])) % 2
            keep, give = first + upper * length, first + (1 - upper) * length
            starts[side].append(keep)
            base = side * quarter + quarter - 2 * length
            half_out[pl.ds(base, length), :] = total[pl.ds(give, length), :].astype(jnp.bfloat16)
            reduce_copy(stage, side).start()
        mass_send(stage + 1)

    def reduce_take(stage):
        length = quarter >> (stage + 1)
        for side in range(2):
            base = side * quarter + quarter - 2 * length
            reduce_copy(stage, side).wait()
            total[pl.ds(starts[side][stage + 1], length), :] += half_in[
                pl.ds(base, length), :
            ].astype(jnp.float32)
        mass_take(stage + 1)

    def spread_copy(stage, side):
        length = quarter >> (stage + 1)
        block = state_ref.at[pl.ds(starts[side][stage + 1], length)]
        slot = 2 + 3 * levels + 2 * stage + side
        return pltpu.make_async_remote_copy(
            src_ref=block, dst_ref=block, send_sem=s_send.at[slot], recv_sem=s_recv.at[slot],
            device_id=to_lane(orders(side)[stage] + 1), device_id_type=MESH,
        )

    final_copy = pltpu.make_async_remote_copy(
        src_ref=state_ref.at[mine], dst_ref=state_ref.at[mine],
        send_sem=s_send.at[2 + 5 * levels], recv_sem=s_recv.at[2 + 5 * levels],
        device_id=to_lane(0), device_id_type=MESH,
    )

    todo = [(k, stage) for k in near[:2] for stage in range(1)]
    later = [(k, 0) for k in near[2:]]
    for stage in range(1, levels + 1):
        later += [(k, stage) for k in near]
    todo += later

    def next_w(amount=1):
        for _ in range(amount):
            if todo:
                w_step(*todo.pop(0))

    for stage in range(levels):
        reduce_send(stage)
        next_w()
        reduce_take(stage)
    length = quarter >> levels
    for side in range(2):
        at = pl.ds(starts[side][levels], length)
        state_ref[at, :] = (total[at, :] / count).astype(jnp.bfloat16)
    mass_ref[...] = sums[...] / count
    for stage in reversed(range(levels)):
        for side in range(2):
            spread_copy(stage, side).start()
        next_w()
        for side in range(2):
            spread_copy(stage, side).wait()
    final_copy.start()
    next_w(len(todo))
    final_copy.wait()
    for k in near:
        z_copy(k).wait_send()
        for stage in range(levels + 1):
            for copy in w_copies(k, stage):
                copy.wait_send()
                if stage == levels:
                    copy.wait_recv()
    own.wait()


def gather(queries, keys_in, values_in, out_weight, count):
    batch, tokens, heads, size = keys_in.shape
    depth, lanes = lax.axis_size("dp"), lax.axis_size("sp")
    places = lanes // 2
    levels = places.bit_length() - 1
    rows, width = out_weight.shape
    area = batch * heads * size
    chunk = min(CHUNK, tokens)
    any_space = pl.BlockSpec(memory_space=pl.ANY)
    vmem = pl.BlockSpec(memory_space=pltpu.VMEM)
    dma = pltpu.SemaphoreType.DMA
    f32, bf16 = jnp.float32, jnp.bfloat16
    return pl.pallas_call(
        functools.partial(
            gather_kernel, (depth, lanes), count, chunk, batch, tokens, heads, size
        ),
        out_shape=(
            jax.ShapeDtypeStruct((area, size), bf16),
            jax.ShapeDtypeStruct((batch * heads, size), f32),
            jax.ShapeDtypeStruct((depth * rows, width), bf16),
        ),
        in_specs=[any_space, any_space, vmem],
        out_specs=(vmem, vmem, any_space),
        scratch_shapes=[
            pltpu.VMEM((SLOTS, chunk, heads, size), bf16),
            pltpu.VMEM((SLOTS, chunk, heads, size), bf16),
            pltpu.VMEM((area, size), f32),
            pltpu.VMEM((batch * heads, size), f32),
            pltpu.VMEM((area // 2, size), f32),
            pltpu.VMEM((area // 2, size), bf16),
            pltpu.VMEM((area // 2, size), bf16),
            pltpu.VMEM((levels + 1, batch * heads, size), f32),
            pltpu.VMEM((levels + 1, batch * heads, size), f32),
            dma((2, SLOTS)),
            dma,
            dma((depth,)),
            dma((depth,)),
            dma((depth, 2 * places - 1)),
            dma((depth, 2 * places - 1)),
            dma((3 + 5 * levels,)),
            dma((3 + 5 * levels,)),
        ],
        compiler_params=pltpu.CompilerParams(
            collective_id=0, has_side_effects=True, vmem_limit_bytes=60 * 2**20
        ),
    )(keys_in, values_in, out_weight)


def project_kernel(count, q_ref, state_ref, mass_ref, w_ref, out_ref, table, mixed):
    heads, size = q_ref.shape[2:]
    tile = q_ref.shape[1]
    f32, bf16 = jnp.float32, jnp.bfloat16

    @pl.when(pl.program_id(1) == 0)
    def _():
        b = pl.program_id(0)
        for h in range(heads):
            line = mass_ref[pl.ds(b * heads + h, 1), :]
            column = jnp.transpose(jnp.broadcast_to(line, (size, size)))
            high = column.astype(bf16)
            table[h, :size, :size] = state_ref[pl.ds((b * heads + h) * size, size), :]
            table[h, :size, size:] = high
            table[h, size:, :size] = jnp.zeros((size, size), bf16)
            table[h, size:, size:] = (column - high.astype(f32)).astype(bf16)

    q_heads = pltpu.einshape("thd->htd", feature_map(q_ref[0]))
    for h in range(heads):
        feature = q_heads[h]
        both = jnp.dot(
            jnp.concatenate([feature, feature], axis=1), table[h], preferred_element_type=f32
        )
        read = both[:, :size] / (both[:, size:] + 0.001)
        mixed[:, h * size : (h + 1) * size] = (read * count**0.5).astype(bf16)
    out_ref[0] = jnp.dot(mixed[...], w_ref[...], preferred_element_type=f32).astype(bf16)


def project(queries_in, state, mass, wide, count):
    batch, tokens, heads, size = queries_in.shape
    width = wide.shape[1]
    tile = min(TILE, tokens)
    return pl.pallas_call(
        functools.partial(project_kernel, count),
        grid=(batch, tokens // tile),
        out_shape=jax.ShapeDtypeStruct((batch, tokens, width), jnp.bfloat16),
        in_specs=[
            pl.BlockSpec((1, tile, heads, size), lambda b, t: (b, t, 0, 0)),
            pl.BlockSpec(memory_space=pltpu.VMEM),
            pl.BlockSpec(memory_space=pltpu.VMEM),
            pl.BlockSpec(memory_space=pltpu.VMEM),
        ],
        out_specs=pl.BlockSpec((1, tile, width), lambda b, t: (b, t, 0)),
        scratch_shapes=[
            pltpu.VMEM((heads, 2 * size, 2 * size), jnp.bfloat16),
            pltpu.VMEM((tile, heads * size), jnp.bfloat16),
        ],
        compiler_params=pltpu.CompilerParams(
            dimension_semantics=("arbitrary", "arbitrary"), vmem_limit_bytes=60 * 2**20
        ),
    )(queries_in, state, mass, wide)


def on_device(queries_in, keys_in, values_in, out_weight):
    count = queries_in.shape[1] * lax.axis_size("sp")
    state, mass, wide = gather(queries_in, keys_in, values_in, out_weight, count)
    return project(queries_in, state, mass, wide, count)


def solution(mesh):
    placed = (
        P("dp", "sp", None, None),
        P("dp", "sp", None, None),
        P("dp", "sp", None, None),
        P("dp", None),
    )
    return jax.shard_map(
        on_device, mesh=mesh, in_specs=placed, out_specs=P("dp", "sp", None), check_vma=False
    )
```

```python
import functools

import jax
import jax.numpy as jnp
from jax import lax
from jax.experimental import pallas as pl
from jax.experimental.pallas import tpu as pltpu
from jax.sharding import PartitionSpec as P

MESH = pl.DeviceIdType.MESH
SLOTS = 3
CHUNK = 256
TILE = 256


def feature_map(values):
    wide = values.astype(jnp.float32)
    return (wide * wide + 0.1).astype(jnp.bfloat16)


def gather_kernel(
    groups, count, chunk, batch, tokens, heads, size,
    k_ref, v_ref, w_ref, state_ref, mass_ref, wide_ref,
    k_buf, v_buf, total, sums, core_in, half_out, half_in, sums_out, sums_in,
    load_sem, own_sem, z_send, z_recv, w_send, w_recv, s_send, s_recv,
):
    depth, lanes = groups
    places = lanes // 2
    levels = places.bit_length() - 1
    d, s = lax.axis_index("dp"), lax.axis_index("sp")
    core, place = s % 2, s // 2
    piece = core * places + place
    rows = w_ref.shape[0]
    part = rows // lanes
    half_width = w_ref.shape[1] // 2
    steps = batch * tokens // chunk
    per_batch = tokens // chunk

    def flip(value, bit):
        return value + (1 << bit) - 2 * (1 << bit) * ((value // (1 << bit)) % 2)

    partners = [flip(s, bit) for bit in range(levels + 1)]

    def to_lane(bit):
        return {"sp": partners[bit]}

    barrier = pltpu.get_barrier_semaphore()
    for bit in range(levels + 1):
        pl.semaphore_signal(barrier, inc=1, device_id=to_lane(bit), device_id_type=MESH)
    for k in (1, depth - 1):
        pl.semaphore_signal(
            barrier, inc=1, device_id={"dp": (d + k) % depth}, device_id_type=MESH
        )

    def load(i):
        half = steps // 2
        side = jnp.where(i < half, 1 - core, core)
        at = side * half + i % half
        b, t = at // per_batch, at % per_batch
        slot = i % SLOTS
        return (
            pltpu.make_async_copy(
                k_ref.at[b, pl.ds(t * chunk, chunk)], k_buf.at[slot], load_sem.at[0, slot]
            ),
            pltpu.make_async_copy(
                v_ref.at[b, pl.ds(t * chunk, chunk)], v_buf.at[slot], load_sem.at[1, slot]
            ),
        )

    for i in range(min(SLOTS - 1, steps)):
        for copy in load(i):
            copy.start()
    total[...] = jnp.zeros_like(total)
    sums[...] = jnp.zeros_like(sums)
    pl.semaphore_wait(barrier, levels + 3)

    def origin(way, hop):
        return d - hop if way == 0 else d + hop

    def inside(place_on_dp):
        return jnp.logical_and(place_on_dp >= 0, place_on_dp < depth)

    def z_copy(way, hop):
        at = pl.ds(origin(way, hop - 1) * rows + piece * part, part)
        return pltpu.make_async_remote_copy(
            src_ref=w_ref.at[pl.ds(piece * part, part)] if hop == 1 else wide_ref.at[at],
            dst_ref=wide_ref.at[at],
            send_sem=z_send.at[way, hop],
            recv_sem=z_recv.at[way, hop],
            device_id={"dp": (d + (1 if way == 0 else depth - 1)) % depth},
            device_id_type=MESH,
        )

    def sends(way, hop):
        return jnp.logical_and(inside(origin(way, hop - 1)), inside(origin(way, -1)))

    def z_start(hop):
        for way in range(2):
            pl.when(sends(way, hop))(lambda way=way: z_copy(way, hop).start())

    z_start(1)
    own = pltpu.make_async_copy(w_ref, wide_ref.at[pl.ds(d * rows, rows)], own_sem)
    own.start()

    def orders(side):
        return list(range(levels)) if side == 0 else list(range(levels))[::-1]

    def w_copies(way, hop, stage):
        first = origin(way, hop) * rows
        k = way * depth + hop
        if stage == levels:
            block = wide_ref.at[pl.ds(first + core * places * part, places * part)]
            slot = 2 * (places - 1)
            return [
                pltpu.make_async_remote_copy(
                    src_ref=block, dst_ref=block, send_sem=w_send.at[k, slot],
                    recv_sem=w_recv.at[k, slot], device_id=to_lane(0), device_id_type=MESH,
                )
            ]
        copies = []
        for side in range(2):
            bits = orders(side)
            for subset in range(1 << stage):
                member = place
                for j in range(stage):
                    if subset >> j & 1:
                        member = flip(member, bits[j])
                slot = side * (places - 1) + (1 << stage) - 1 + subset
                block = wide_ref.at[
                    pl.ds(first + (core * places + member) * part, part),
                    pl.ds(side * half_width, half_width),
                ]
                copies.append(
                    pltpu.make_async_remote_copy(
                        src_ref=block, dst_ref=block, send_sem=w_send.at[k, slot],
                        recv_sem=w_recv.at[k, slot], device_id=to_lane(bits[stage] + 1),
                        device_id_type=MESH,
                    )
                )
        return copies

    def w_step(hop, stage):
        def arrived(way):
            if stage == 0:
                at = pl.ds(origin(way, hop) * rows + piece * part, part)
                pltpu.make_async_remote_copy(
                    src_ref=wide_ref.at[at], dst_ref=wide_ref.at[at],
                    send_sem=z_send.at[way, hop], recv_sem=z_recv.at[way, hop],
                    device_id={"dp": (d + 1) % depth}, device_id_type=MESH,
                ).wait_recv()
            else:
                for copy in w_copies(way, hop, stage - 1):
                    copy.wait_recv()

        def forward(way):
            for copy in w_copies(way, hop, stage):
                copy.start()

        for act in (arrived, None, forward):
            if act is None:
                if stage == 0 and hop + 1 < depth:
                    z_start(hop + 1)
                continue
            for way in range(2):
                pl.when(inside(origin(way, hop)))(functools.partial(act, way))

    todo = [(hop, stage) for hop in range(1, depth) for stage in range(levels + 1)]
    todo.sort(key=lambda item: (item[0] + item[1], item[0]))
    early = {steps // 2: todo.pop(0), steps - 2: todo.pop(0), steps - 1: todo.pop(0)}

    held = total.shape[0] // 2
    core_copy = pltpu.make_async_remote_copy(
        src_ref=total.at[pl.ds((1 - core) * held, held)], dst_ref=core_in,
        send_sem=s_send.at[0], recv_sem=s_recv.at[0],
        device_id=to_lane(0), device_id_type=MESH,
    )

    def step(i, carry):
        @pl.when(i + SLOTS - 1 < steps)
        def _():
            for copy in load(i + SLOTS - 1):
                copy.start()

        @pl.when(i == steps // 2)
        def _():
            core_copy.start()

        for moment, item in early.items():
            pl.when(i == moment)(functools.partial(w_step, *item))

        for copy in load(i):
            copy.wait()
        slot = i % SLOTS
        half = steps // 2
        b = (jnp.where(i < half, 1 - core, core) * half + i % half) // per_batch
        k_feature = feature_map(k_buf[slot])
        sums[pl.ds(b * heads, heads), :] += jnp.sum(k_feature.astype(jnp.float32), axis=0)
        k_heads = pltpu.einshape("thd->htd", k_feature)
        v_heads = pltpu.einshape("thd->htd", v_buf[slot])
        for h in range(heads):
            at = pl.ds((b * heads + h) * size, size)
            total[at, :] += lax.dot_general(
                k_heads[h], v_heads[h], (((0,), (0,)), ((), ())),
                preferred_element_type=jnp.float32,
            )
        return carry

    lax.fori_loop(0, steps, step, 0)

    def mass_copy(stage):
        bit = 0 if stage == 0 else orders(0)[stage - 1] + 1
        return pltpu.make_async_remote_copy(
            src_ref=sums_out.at[stage], dst_ref=sums_in.at[stage],
            send_sem=s_send.at[1 + stage], recv_sem=s_recv.at[1 + stage],
            device_id=to_lane(bit), device_id_type=MESH,
        )

    def mass_send(stage):
        sums_out[stage] = sums[...]
        mass_copy(stage).start()

    def mass_take(stage):
        mass_copy(stage).wait()
        sums[...] += sums_in[stage]

    mass_send(0)
    core_copy.wait()
    mine = pl.ds(core * held, held)
    total[mine, :] += core_in[...]
    mass_take(0)

    quarter = held // 2
    starts = [[core * held + side * quarter] for side in range(2)]

    def reduce_copy(stage, side):
        length = quarter >> (stage + 1)
        slot = 2 + levels + 2 * stage + side
        base = side * quarter + quarter - 2 * length
        return pltpu.make_async_remote_copy(
            src_ref=half_out.at[pl.ds(base, length)], dst_ref=half_in.at[pl.ds(base, length)],
            send_sem=s_send.at[slot], recv_sem=s_recv.at[slot],
            device_id=to_lane(orders(side)[stage] + 1), device_id_type=MESH,
        )

    def reduce_send(stage):
        length = quarter >> (stage + 1)
        for side in range(2):
            first = starts[side][stage]
            upper = (place // (1 << orders(side)[stage])) % 2
            keep, give = first + upper * length, first + (1 - upper) * length
            starts[side].append(keep)
            base = side * quarter + quarter - 2 * length
            half_out[pl.ds(base, length), :] = total[pl.ds(give, length), :].astype(jnp.bfloat16)
            reduce_copy(stage, side).start()
        mass_send(stage + 1)

    def reduce_take(stage):
        length = quarter >> (stage + 1)
        for side in range(2):
            base = side * quarter + quarter - 2 * length
            reduce_copy(stage, side).wait()
            total[pl.ds(starts[side][stage + 1], length), :] += half_in[
                pl.ds(base, length), :
            ].astype(jnp.float32)
        mass_take(stage + 1)

    def spread_copy(stage, side):
        length = quarter >> (stage + 1)
        block = state_ref.at[pl.ds(starts[side][stage + 1], length)]
        slot = 2 + 3 * levels + 2 * stage + side
        return pltpu.make_async_remote_copy(
            src_ref=block, dst_ref=block, send_sem=s_send.at[slot], recv_sem=s_recv.at[slot],
            device_id=to_lane(orders(side)[stage] + 1), device_id_type=MESH,
        )

    final_copy = pltpu.make_async_remote_copy(
        src_ref=state_ref.at[mine], dst_ref=state_ref.at[mine],
        send_sem=s_send.at[2 + 5 * levels], recv_sem=s_recv.at[2 + 5 * levels],
        device_id=to_lane(0), device_id_type=MESH,
    )

    def next_w(amount=1):
        for _ in range(amount):
            if todo:
                w_step(*todo.pop(0))

    for stage in range(levels):
        reduce_send(stage)
        next_w(2 - stage)
        reduce_take(stage)
    length = quarter >> levels
    for side in range(2):
        at = pl.ds(starts[side][levels], length)
        state_ref[at, :] = (total[at, :] / count).astype(jnp.bfloat16)
    mass_ref[...] = sums[...] / count
    for stage in reversed(range(levels)):
        for side in range(2):
            spread_copy(stage, side).start()
        next_w()
        for side in range(2):
            spread_copy(stage, side).wait()
    final_copy.start()
    next_w(len(todo))
    final_copy.wait()
    for hop in range(1, depth):
        for way in range(2):
            pl.when(sends(way, hop))(lambda way=way, hop=hop: z_copy(way, hop).wait_send())

            @pl.when(inside(origin(way, hop)))
            def _(way=way, hop=hop):
                for stage in range(levels + 1):
                    for copy in w_copies(way, hop, stage):
                        copy.wait_send()
                        if stage == levels:
                            copy.wait_recv()

    own.wait()


def gather(queries, keys_in, values_in, out_weight, count):
    batch, tokens, heads, size = keys_in.shape
    depth, lanes = lax.axis_size("dp"), lax.axis_size("sp")
    places = lanes // 2
    levels = places.bit_length() - 1
    rows, width = out_weight.shape
    area = batch * heads * size
    chunk = min(CHUNK, tokens)
    any_space = pl.BlockSpec(memory_space=pl.ANY)
    vmem = pl.BlockSpec(memory_space=pltpu.VMEM)
    dma = pltpu.SemaphoreType.DMA
    f32, bf16 = jnp.float32, jnp.bfloat16
    return pl.pallas_call(
        functools.partial(
            gather_kernel, (depth, lanes), count, chunk, batch, tokens, heads, size
        ),
        out_shape=(
            jax.ShapeDtypeStruct((area, size), bf16),
            jax.ShapeDtypeStruct((batch * heads, size), f32),
            jax.ShapeDtypeStruct((depth * rows, width), bf16),
        ),
        in_specs=[any_space, any_space, vmem],
        out_specs=(vmem, vmem, any_space),
        scratch_shapes=[
            pltpu.VMEM((SLOTS, chunk, heads, size), bf16),
            pltpu.VMEM((SLOTS, chunk, heads, size), bf16),
            pltpu.VMEM((area, size), f32),
            pltpu.VMEM((batch * heads, size), f32),
            pltpu.VMEM((area // 2, size), f32),
            pltpu.VMEM((area // 2, size), bf16),
            pltpu.VMEM((area // 2, size), bf16),
            pltpu.VMEM((levels + 1, batch * heads, size), f32),
            pltpu.VMEM((levels + 1, batch * heads, size), f32),
            dma((2, SLOTS)),
            dma,
            dma((2, depth)),
            dma((2, depth)),
            dma((2 * depth, 2 * places - 1)),
            dma((2 * depth, 2 * places - 1)),
            dma((3 + 5 * levels,)),
            dma((3 + 5 * levels,)),
        ],
        compiler_params=pltpu.CompilerParams(
            collective_id=0, has_side_effects=True, vmem_limit_bytes=60 * 2**20
        ),
    )(keys_in, values_in, out_weight)


def project_kernel(
    count, per_batch, q_ref, state_ref, mass_ref, w_hbm, out_ref, table, mixed, w_ref, w_sem
):
    heads, size = q_ref.shape[1:]
    f32, bf16 = jnp.float32, jnp.bfloat16
    i, last = pl.program_id(0), pl.num_programs(0) - 1
    load = pltpu.make_async_copy(w_hbm, w_ref, w_sem)

    pl.when(i == 0)(load.start)

    @pl.when(jnp.logical_and(i % per_batch == 0, i < last))
    def _():
        b = i // per_batch
        for h in range(heads):
            line = mass_ref[pl.ds(b * heads + h, 1), :]
            column = jnp.transpose(jnp.broadcast_to(line, (size, size)))
            high = column.astype(bf16)
            table[h, :size, :size] = state_ref[pl.ds((b * heads + h) * size, size), :]
            table[h, :size, size:] = high
            table[h, size:, :size] = jnp.zeros((size, size), bf16)
            table[h, size:, size:] = (column - high.astype(f32)).astype(bf16)

    def read(slot):
        q_heads = pltpu.einshape("thd->htd", feature_map(q_ref[...]))
        for h in range(heads):
            feature = q_heads[h]
            both = jnp.dot(
                jnp.concatenate([feature, feature], axis=1), table[h], preferred_element_type=f32
            )
            top = both[:, :size] / (both[:, size:] + 0.001)
            mixed[slot, :, h * size : (h + 1) * size] = (top * count**0.5).astype(bf16)

    def finish(slot):
        out_ref[...] = jnp.dot(mixed[slot], w_ref[...], preferred_element_type=f32).astype(bf16)

    @pl.when(i == 0)
    def _():
        read(0)
        load.wait()

    for slot in range(2):
        @pl.when(jnp.logical_and(i % 2 == slot, jnp.logical_and(i > 0, i < last)))
        def _():
            finish(1 - slot)
            read(slot)

        @pl.when(jnp.logical_and(i % 2 == slot, i == last))
        def _():
            finish(1 - slot)


def project(queries_in, state, mass, wide, count):
    batch, tokens, heads, size = queries_in.shape
    width = wide.shape[1]
    tile = min(TILE, tokens)
    tiles = batch * tokens // tile
    vmem = pl.BlockSpec(memory_space=pltpu.VMEM)
    out = pl.pallas_call(
        functools.partial(project_kernel, count, tokens // tile),
        grid=(tiles + 1,),
        out_shape=jax.ShapeDtypeStruct((batch * tokens, width), jnp.bfloat16),
        in_specs=[
            pl.BlockSpec((tile, heads, size), lambda i: (jnp.minimum(i, tiles - 1), 0, 0)),
            vmem,
            vmem,
            pl.BlockSpec(memory_space=pl.ANY),
        ],
        out_specs=pl.BlockSpec((tile, width), lambda i: (jnp.maximum(i - 1, 0), 0)),
        scratch_shapes=[
            pltpu.VMEM((heads, 2 * size, 2 * size), jnp.bfloat16),
            pltpu.VMEM((2, tile, heads * size), jnp.bfloat16),
            pltpu.VMEM(wide.shape, jnp.bfloat16),
            pltpu.SemaphoreType.DMA,
        ],
        compiler_params=pltpu.CompilerParams(
            dimension_semantics=("arbitrary",), vmem_limit_bytes=60 * 2**20
        ),
    )(queries_in.reshape(batch * tokens, heads, size), state, mass, wide)
    return out.reshape(batch, tokens, width)


def on_device(queries_in, keys_in, values_in, out_weight):
    count = queries_in.shape[1] * lax.axis_size("sp")
    state, mass, wide = gather(queries_in, keys_in, values_in, out_weight, count)
    return project(queries_in, state, mass, wide, count)


def solution(mesh):
    placed = (
        P("dp", "sp", None, None),
        P("dp", "sp", None, None),
        P("dp", "sp", None, None),
        P("dp", None),
    )
    return jax.shard_map(
        on_device, mesh=mesh, in_specs=placed, out_specs=P("dp", "sp", None), check_vma=False
    )
```

```python
import functools

import jax
import jax.numpy as jnp
from jax import lax
from jax.experimental import pallas as pl
from jax.experimental.pallas import tpu as pltpu
from jax.sharding import PartitionSpec as P

MESH = pl.DeviceIdType.MESH
SLOTS = 3
CHUNK = 256
TILE = 512


def feature_map(values):
    wide = values.astype(jnp.float32)
    return (wide * wide + 0.1).astype(jnp.bfloat16)


def gather_kernel(
    groups, count, chunk, batch, tokens, heads, size,
    k_ref, v_ref, w_ref, state_ref, mass_ref, wide_ref,
    k_buf, v_buf, total, sums, core_in, half_out, half_in, sums_out, sums_in,
    load_sem, own_sem, z_send, z_recv, w_send, w_recv, s_send, s_recv,
):
    depth, lanes = groups
    places = lanes // 2
    levels = places.bit_length() - 1
    d, s = lax.axis_index("dp"), lax.axis_index("sp")
    core, place = s % 2, s // 2
    piece = core * places + place
    rows = w_ref.shape[0]
    part = rows // lanes
    half_width = w_ref.shape[1] // 2
    steps = batch * tokens // chunk
    per_batch = tokens // chunk

    def flip(value, bit):
        return value + (1 << bit) - 2 * (1 << bit) * ((value // (1 << bit)) % 2)

    partners = [flip(s, bit) for bit in range(levels + 1)]

    def to_lane(bit):
        return {"sp": partners[bit]}

    barrier = pltpu.get_barrier_semaphore()
    for bit in range(levels + 1):
        pl.semaphore_signal(barrier, inc=1, device_id=to_lane(bit), device_id_type=MESH)
    for k in (1, depth - 1):
        pl.semaphore_signal(
            barrier, inc=1, device_id={"dp": (d + k) % depth}, device_id_type=MESH
        )

    def load(i):
        half = steps // 2
        side = jnp.where(i < half, 1 - core, core)
        at = side * half + i % half
        b, t = at // per_batch, at % per_batch
        slot = i % SLOTS
        return (
            pltpu.make_async_copy(
                k_ref.at[b, pl.ds(t * chunk, chunk)], k_buf.at[slot], load_sem.at[0, slot]
            ),
            pltpu.make_async_copy(
                v_ref.at[b, pl.ds(t * chunk, chunk)], v_buf.at[slot], load_sem.at[1, slot]
            ),
        )

    for i in range(min(SLOTS - 1, steps)):
        for copy in load(i):
            copy.start()
    total[...] = jnp.zeros_like(total)
    sums[...] = jnp.zeros_like(sums)
    pl.semaphore_wait(barrier, levels + 3)

    def origin(way, hop):
        return d - hop if way == 0 else d + hop

    def inside(place_on_dp):
        return jnp.logical_and(place_on_dp >= 0, place_on_dp < depth)

    def z_copy(way, hop):
        at = pl.ds(origin(way, hop - 1) * rows + piece * part, part)
        return pltpu.make_async_remote_copy(
            src_ref=w_ref.at[pl.ds(piece * part, part)] if hop == 1 else wide_ref.at[at],
            dst_ref=wide_ref.at[at],
            send_sem=z_send.at[way, hop],
            recv_sem=z_recv.at[way, hop],
            device_id={"dp": (d + (1 if way == 0 else depth - 1)) % depth},
            device_id_type=MESH,
        )

    def sends(way, hop):
        return jnp.logical_and(inside(origin(way, hop - 1)), inside(origin(way, -1)))

    def z_start(hop):
        for way in range(2):
            pl.when(sends(way, hop))(lambda way=way: z_copy(way, hop).start())

    z_start(1)
    own = pltpu.make_async_copy(w_ref, wide_ref.at[pl.ds(d * rows, rows)], own_sem)
    own.start()

    def orders(side):
        return list(range(levels)) if side == 0 else list(range(levels))[::-1]

    def w_copies(way, hop, stage):
        first = origin(way, hop) * rows
        k = way * depth + hop
        if stage == levels:
            block = wide_ref.at[pl.ds(first + core * places * part, places * part)]
            slot = 2 * (places - 1)
            return [
                pltpu.make_async_remote_copy(
                    src_ref=block, dst_ref=block, send_sem=w_send.at[k, slot],
                    recv_sem=w_recv.at[k, slot], device_id=to_lane(0), device_id_type=MESH,
                )
            ]
        copies = []
        for side in range(2):
            bits = orders(side)
            for subset in range(1 << stage):
                member = place
                for j in range(stage):
                    if subset >> j & 1:
                        member = flip(member, bits[j])
                slot = side * (places - 1) + (1 << stage) - 1 + subset
                block = wide_ref.at[
                    pl.ds(first + (core * places + member) * part, part),
                    pl.ds(side * half_width, half_width),
                ]
                copies.append(
                    pltpu.make_async_remote_copy(
                        src_ref=block, dst_ref=block, send_sem=w_send.at[k, slot],
                        recv_sem=w_recv.at[k, slot], device_id=to_lane(bits[stage] + 1),
                        device_id_type=MESH,
                    )
                )
        return copies

    def w_step(hop, stage):
        def arrived(way):
            if stage == 0:
                at = pl.ds(origin(way, hop) * rows + piece * part, part)
                pltpu.make_async_remote_copy(
                    src_ref=wide_ref.at[at], dst_ref=wide_ref.at[at],
                    send_sem=z_send.at[way, hop], recv_sem=z_recv.at[way, hop],
                    device_id={"dp": (d + 1) % depth}, device_id_type=MESH,
                ).wait_recv()
            else:
                for copy in w_copies(way, hop, stage - 1):
                    copy.wait_recv()

        def forward(way):
            for copy in w_copies(way, hop, stage):
                copy.start()

        for act in (arrived, None, forward):
            if act is None:
                if stage == 0 and hop + 1 < depth:
                    z_start(hop + 1)
                continue
            for way in range(2):
                pl.when(inside(origin(way, hop)))(functools.partial(act, way))

    todo = [(hop, stage) for hop in range(1, depth) for stage in range(levels + 1)]
    todo.sort(key=lambda item: (item[0] + item[1], item[0]))
    early = {steps // 2: todo.pop(0), steps - 2: todo.pop(0), steps - 1: todo.pop(0)}

    held = total.shape[0] // 2
    core_copy = pltpu.make_async_remote_copy(
        src_ref=total.at[pl.ds((1 - core) * held, held)], dst_ref=core_in,
        send_sem=s_send.at[0], recv_sem=s_recv.at[0],
        device_id=to_lane(0), device_id_type=MESH,
    )

    def step(i, carry):
        @pl.when(i + SLOTS - 1 < steps)
        def _():
            for copy in load(i + SLOTS - 1):
                copy.start()

        @pl.when(i == steps // 2)
        def _():
            core_copy.start()

        for moment, item in early.items():
            pl.when(i == moment)(functools.partial(w_step, *item))

        for copy in load(i):
            copy.wait()
        slot = i % SLOTS
        half = steps // 2
        b = (jnp.where(i < half, 1 - core, core) * half + i % half) // per_batch
        k_feature = feature_map(k_buf[slot])
        sums[pl.ds(b * heads, heads), :] += jnp.sum(k_feature.astype(jnp.float32), axis=0)
        k_heads = pltpu.einshape("thd->htd", k_feature)
        v_heads = pltpu.einshape("thd->htd", v_buf[slot])
        for h in range(heads):
            at = pl.ds((b * heads + h) * size, size)
            total[at, :] += lax.dot_general(
                k_heads[h], v_heads[h], (((0,), (0,)), ((), ())),
                preferred_element_type=jnp.float32,
            )
        return carry

    lax.fori_loop(0, steps, step, 0)

    def mass_copy(stage):
        bit = 0 if stage == 0 else orders(0)[stage - 1] + 1
        return pltpu.make_async_remote_copy(
            src_ref=sums_out.at[stage], dst_ref=sums_in.at[stage],
            send_sem=s_send.at[1 + stage], recv_sem=s_recv.at[1 + stage],
            device_id=to_lane(bit), device_id_type=MESH,
        )

    def mass_send(stage):
        sums_out[stage] = sums[...]
        mass_copy(stage).start()

    def mass_take(stage):
        mass_copy(stage).wait()
        sums[...] += sums_in[stage]

    mass_send(0)
    core_copy.wait()
    mine = pl.ds(core * held, held)
    total[mine, :] += core_in[...]
    mass_take(0)

    quarter = held // 2
    starts = [[core * held + side * quarter] for side in range(2)]

    def reduce_copy(stage, side):
        length = quarter >> (stage + 1)
        slot = 2 + levels + 2 * stage + side
        base = side * quarter + quarter - 2 * length
        return pltpu.make_async_remote_copy(
            src_ref=half_out.at[pl.ds(base, length)], dst_ref=half_in.at[pl.ds(base, length)],
            send_sem=s_send.at[slot], recv_sem=s_recv.at[slot],
            device_id=to_lane(orders(side)[stage] + 1), device_id_type=MESH,
        )

    def reduce_send(stage):
        length = quarter >> (stage + 1)
        for side in range(2):
            first = starts[side][stage]
            upper = (place // (1 << orders(side)[stage])) % 2
            keep, give = first + upper * length, first + (1 - upper) * length
            starts[side].append(keep)
            base = side * quarter + quarter - 2 * length
            half_out[pl.ds(base, length), :] = total[pl.ds(give, length), :].astype(jnp.bfloat16)
            reduce_copy(stage, side).start()
        mass_send(stage + 1)

    def reduce_take(stage):
        length = quarter >> (stage + 1)
        for side in range(2):
            base = side * quarter + quarter - 2 * length
            reduce_copy(stage, side).wait()
            total[pl.ds(starts[side][stage + 1], length), :] += half_in[
                pl.ds(base, length), :
            ].astype(jnp.float32)
        mass_take(stage + 1)

    def spread_copy(stage, side):
        length = quarter >> (stage + 1)
        block = state_ref.at[pl.ds(starts[side][stage + 1], length)]
        slot = 2 + 3 * levels + 2 * stage + side
        return pltpu.make_async_remote_copy(
            src_ref=block, dst_ref=block, send_sem=s_send.at[slot], recv_sem=s_recv.at[slot],
            device_id=to_lane(orders(side)[stage] + 1), device_id_type=MESH,
        )

    final_copy = pltpu.make_async_remote_copy(
        src_ref=state_ref.at[mine], dst_ref=state_ref.at[mine],
        send_sem=s_send.at[2 + 5 * levels], recv_sem=s_recv.at[2 + 5 * levels],
        device_id=to_lane(0), device_id_type=MESH,
    )

    def next_w(amount=1):
        for _ in range(amount):
            if todo:
                w_step(*todo.pop(0))

    for stage in range(levels):
        reduce_send(stage)
        next_w(2 - stage)
        reduce_take(stage)
    length = quarter >> levels
    for side in range(2):
        at = pl.ds(starts[side][levels], length)
        state_ref[at, :] = (total[at, :] / count).astype(jnp.bfloat16)
    mass_ref[...] = sums[...] / count
    for stage in reversed(range(levels)):
        for side in range(2):
            spread_copy(stage, side).start()
        next_w()
        for side in range(2):
            spread_copy(stage, side).wait()
    final_copy.start()
    next_w(len(todo))
    final_copy.wait()
    for hop in range(1, depth):
        for way in range(2):
            pl.when(sends(way, hop))(lambda way=way, hop=hop: z_copy(way, hop).wait_send())

            @pl.when(inside(origin(way, hop)))
            def _(way=way, hop=hop):
                for stage in range(levels + 1):
                    for copy in w_copies(way, hop, stage):
                        copy.wait_send()
                        if stage == levels:
                            copy.wait_recv()

    own.wait()


def gather(queries, keys_in, values_in, out_weight, count):
    batch, tokens, heads, size = keys_in.shape
    depth, lanes = lax.axis_size("dp"), lax.axis_size("sp")
    places = lanes // 2
    levels = places.bit_length() - 1
    rows, width = out_weight.shape
    area = batch * heads * size
    chunk = min(CHUNK, tokens)
    any_space = pl.BlockSpec(memory_space=pl.ANY)
    vmem = pl.BlockSpec(memory_space=pltpu.VMEM)
    dma = pltpu.SemaphoreType.DMA
    f32, bf16 = jnp.float32, jnp.bfloat16
    return pl.pallas_call(
        functools.partial(
            gather_kernel, (depth, lanes), count, chunk, batch, tokens, heads, size
        ),
        out_shape=(
            jax.ShapeDtypeStruct((area, size), bf16),
            jax.ShapeDtypeStruct((batch * heads, size), f32),
            jax.ShapeDtypeStruct((depth * rows, width), bf16),
        ),
        in_specs=[any_space, any_space, vmem],
        out_specs=(vmem, vmem, any_space),
        scratch_shapes=[
            pltpu.VMEM((SLOTS, chunk, heads, size), bf16),
            pltpu.VMEM((SLOTS, chunk, heads, size), bf16),
            pltpu.VMEM((area, size), f32),
            pltpu.VMEM((batch * heads, size), f32),
            pltpu.VMEM((area // 2, size), f32),
            pltpu.VMEM((area // 2, size), bf16),
            pltpu.VMEM((area // 2, size), bf16),
            pltpu.VMEM((levels + 1, batch * heads, size), f32),
            pltpu.VMEM((levels + 1, batch * heads, size), f32),
            dma((2, SLOTS)),
            dma,
            dma((2, depth)),
            dma((2, depth)),
            dma((2 * depth, 2 * places - 1)),
            dma((2 * depth, 2 * places - 1)),
            dma((3 + 5 * levels,)),
            dma((3 + 5 * levels,)),
        ],
        compiler_params=pltpu.CompilerParams(
            collective_id=0, has_side_effects=True, vmem_limit_bytes=60 * 2**20
        ),
    )(keys_in, values_in, out_weight)


def project_kernel(
    count, per_batch, q_ref, state_ref, mass_ref, w_hbm, out_ref, table, mixed, w_ref, w_sem
):
    heads, size = q_ref.shape[1:]
    f32, bf16 = jnp.float32, jnp.bfloat16
    i, last = pl.program_id(0), pl.num_programs(0) - 1
    load = pltpu.make_async_copy(w_hbm, w_ref, w_sem)

    pl.when(i == 0)(load.start)

    @pl.when(jnp.logical_and(i % per_batch == 0, i < last))
    def _():
        b = i // per_batch
        for h in range(heads):
            line = mass_ref[pl.ds(b * heads + h, 1), :]
            column = jnp.transpose(jnp.broadcast_to(line, (size, size)))
            high = column.astype(bf16)
            table[h, :size, :size] = state_ref[pl.ds((b * heads + h) * size, size), :]
            table[h, :size, size:] = high
            table[h, size:, :size] = jnp.zeros((size, size), bf16)
            table[h, size:, size:] = (column - high.astype(f32)).astype(bf16)

    def read(slot):
        q_heads = pltpu.einshape("thd->htd", feature_map(q_ref[...]))
        for h in range(heads):
            feature = q_heads[h]
            both = jnp.dot(
                jnp.concatenate([feature, feature], axis=1), table[h], preferred_element_type=f32
            )
            top = both[:, :size] / (both[:, size:] + 0.001)
            mixed[slot, :, h * size : (h + 1) * size] = (top * count**0.5).astype(bf16)

    def finish(slot):
        out_ref[...] = jnp.dot(mixed[slot], w_ref[...], preferred_element_type=f32).astype(bf16)

    @pl.when(i == 0)
    def _():
        read(0)
        load.wait()

    for slot in range(2):
        @pl.when(jnp.logical_and(i % 2 == slot, jnp.logical_and(i > 0, i < last)))
        def _():
            finish(1 - slot)
            read(slot)

        @pl.when(jnp.logical_and(i % 2 == slot, i == last))
        def _():
            finish(1 - slot)


def project(queries_in, state, mass, wide, count):
    batch, tokens, heads, size = queries_in.shape
    width = wide.shape[1]
    tile = min(TILE, tokens)
    tiles = batch * tokens // tile
    vmem = pl.BlockSpec(memory_space=pltpu.VMEM)
    out = pl.pallas_call(
        functools.partial(project_kernel, count, tokens // tile),
        grid=(tiles + 1,),
        out_shape=jax.ShapeDtypeStruct((batch * tokens, width), jnp.bfloat16),
        in_specs=[
            pl.BlockSpec((tile, heads, size), lambda i: (jnp.minimum(i, tiles - 1), 0, 0)),
            vmem,
            vmem,
            pl.BlockSpec(memory_space=pl.ANY),
        ],
        out_specs=pl.BlockSpec((tile, width), lambda i: (jnp.maximum(i - 1, 0), 0)),
        scratch_shapes=[
            pltpu.VMEM((heads, 2 * size, 2 * size), jnp.bfloat16),
            pltpu.VMEM((2, tile, heads * size), jnp.bfloat16),
            pltpu.VMEM(wide.shape, jnp.bfloat16),
            pltpu.SemaphoreType.DMA,
        ],
        compiler_params=pltpu.CompilerParams(
            dimension_semantics=("arbitrary",), vmem_limit_bytes=60 * 2**20
        ),
    )(queries_in.reshape(batch * tokens, heads, size), state, mass, wide)
    return out.reshape(batch, tokens, width)


def on_device(queries_in, keys_in, values_in, out_weight):
    count = queries_in.shape[1] * lax.axis_size("sp")
    state, mass, wide = gather(queries_in, keys_in, values_in, out_weight, count)
    return project(queries_in, state, mass, wide, count)


def solution(mesh):
    placed = (
        P("dp", "sp", None, None),
        P("dp", "sp", None, None),
        P("dp", "sp", None, None),
        P("dp", None),
    )
    return jax.shard_map(
        on_device, mesh=mesh, in_specs=placed, out_specs=P("dp", "sp", None), check_vma=False
    )
```
